256 devices in a mesh: row: 16 (over z_hi, x), col: 8 (over y, core), depth: 2 (over z_lo).
Axes of the slice: x: 4, y: 4, z: 8 (z_hi: 4, z_lo: 2; z = z_hi * 2 + z_lo), core: 2. Of those that a mesh axis runs over, the one named last changes fastest.
Arguments:
- volume: bfloat16 [32, 128, 16, 256], P('row', 'col', 'depth'), may hold values from -6 to 6
- first_kernel: bfloat16 [27, 256, 256], P(None, 'row'), may hold values from -0.078125 to 0.078125
- down_kernel: bfloat16 [8, 256, 512], replicated, may hold values from -0.125 to 0.125
- mid_kernel: bfloat16 [27, 512, 512], P(None, None, 'col'), may hold values from -0.0546875 to 0.0546875
- up_kernel: bfloat16 [8, 512, 256], replicated, may hold values from -0.25 to 0.25
- last_kernel: bfloat16 [27, 512, 256], P(None, 'row'), may hold values from -0.0546875 to 0.0546875
Outputs:
- decoded: bfloat16 [32, 128, 16, 256], P('row', 'col', 'depth')
The draws below stay inside these ranges and needn't reach their ends.
All inputs are finite; a program needn't handle non-finite values.
Results may differ from the reference program's by a relative error of at most 0.0055.
Values may be sent and summed in bfloat16 or wider, within the bound.
No kernel may reach another device: no remote copies, remote signals or barrier semaphores. Data moves between devices by JAX's collectives and lax.ppermute only.
A program may use at most 64 MiB of HBM per device.

```python
import jax
import jax.numpy as jnp
from jax import lax

CHANS = 256
WIDE = 512
ROWS = 32
COLS = 128
DEEP = 16


def block_scale(rng, shape, split, low, largest):
    def one(axis_at, parts):
        heights = jax.random.uniform(jax.random.fold_in(jax.random.fold_in(rng, 6), axis_at), (parts,), jnp.float32, low / len(split), largest / len(split))
        return jnp.repeat(jnp.exp(heights), shape[axis_at] // parts).reshape((-1,) + (1,) * (len(shape) - axis_at - 1))

    loudness = one(*split[0])
    for cut in split[1:]:
        loudness = loudness * one(*cut)
    return loudness


def bell_draw(key, extent, width, bound, cuts=(), kind=jnp.bfloat16):
    gain = block_scale(key, extent, cuts, -0.22, 0.18) if cuts else 1.0
    values = jax.random.normal(key, extent, jnp.float32) * width * gain
    return jnp.minimum(jnp.maximum(values, -bound), bound).astype(kind)


def setup_inputs(seed: int = 0) -> dict:
    seeds = jax.random.split(jax.random.key(seed), 7)
    return {
        "volume": bell_draw(seeds[0], (ROWS, COLS, DEEP, CHANS), 1.0, 6.0, ((0, 16), (1, 8), (2, 2))),
        "first_kernel": bell_draw(seeds[1], (27, CHANS, CHANS), (27 * CHANS) ** -0.5, 0.078125, ((1, 16),)),
        "down_kernel": bell_draw(seeds[2], (8, CHANS, WIDE), (8 * CHANS) ** -0.5, 0.125),
        "mid_kernel": bell_draw(seeds[3], (27, WIDE, WIDE), (27 * WIDE) ** -0.5, 0.0546875, ((2, 8),)),
        "up_kernel": bell_draw(seeds[4], (8, WIDE, CHANS), WIDE ** -0.5, 0.25),
        "last_kernel": bell_draw(seeds[5], (27, 2 * CHANS, CHANS), (27 * 2 * CHANS) ** -0.5, 0.0546875, ((1, 16),)),
    }


def conv_same(volume_in, weight):
    kernel = weight.reshape(3, 3, 3, weight.shape[1], weight.shape[2])
    result = lax.conv_general_dilated(volume_in[None], kernel, (1, 1, 1), ((1, 1), (1, 1), (1, 1)), dimension_numbers=("NDHWC", "DHWIO", "NDHWC"), preferred_element_type=jnp.float32)
    return result[0]


def reference(volume, first_kernel, down_kernel, mid_kernel, up_kernel, last_kernel):
    skip = jax.nn.gelu(conv_same(volume, first_kernel)).astype(jnp.bfloat16)
    down_weights = down_kernel.reshape(2, 2, 2, down_kernel.shape[1], down_kernel.shape[2])
    coarse_raw = lax.conv_general_dilated(skip[None], down_weights, (2, 2, 2), "VALID", dimension_numbers=("NDHWC", "DHWIO", "NDHWC"), preferred_element_type=jnp.float32)[0]
    coarse = jax.nn.gelu(coarse_raw).astype(jnp.bfloat16)
    middle = jax.nn.gelu(conv_same(coarse, mid_kernel)).astype(jnp.bfloat16)
    coarse_x, coarse_y, coarse_z, wide_chans = middle.shape
    fine_chans = up_kernel.shape[2]
    up_table = jnp.transpose(up_kernel, (1, 0, 2)).reshape(wide_chans, 8 * fine_chans)
    lifted_flat = jnp.dot(middle.reshape(-1, wide_chans), up_table, preferred_element_type=jnp.float32).astype(jnp.bfloat16)
    lifted = lifted_flat.reshape(coarse_x, coarse_y, coarse_z, 2, 2, 2, fine_chans)
    lifted = jnp.transpose(lifted, (0, 3, 1, 4, 2, 5, 6)).reshape(2 * coarse_x, 2 * coarse_y, 2 * coarse_z, fine_chans)
    joined = jnp.concatenate([lifted, skip], axis=-1)
    return jax.nn.gelu(conv_same(joined, last_kernel)).astype(jnp.bfloat16)
```

```python
import functools

import jax
import jax.numpy as jnp
import numpy as np
from jax import lax
from jax.sharding import PartitionSpec as P

BF = jnp.bfloat16
F32 = jnp.float32
ALL = ("row", "col", "depth")


def shards_of(r, j):
    zhi, x = r // 4, r % 4
    y, c = j // 2, j % 2
    s1 = ((zhi + c) % 4) * 4 + (x + y) % 4
    s2 = ((zhi + c + 2) % 4) * 4 + (x - y) % 4
    return s1, s2


def flat(r, j, d):
    return (r * 8 + j) * 2 + d


def shard_perms():
    p1, p2 = [], []
    for r in range(16):
        for j in range(8):
            for d in range(2):
                s1, s2 = shards_of(r, j)
                p1.append((flat(s1, j, d), flat(r, j, d)))
                p2.append((flat(s2, j, d if j % 2 else 1 - d), flat(r, j, d)))
    return p1, p2


def tables():
    first = np.zeros((16, 256), np.int32)
    skip = np.zeros((16, 256), np.int32)
    for r in range(16):
        for j in range(8):
            s1, s2 = shards_of(r, j)
            sk = (s2 if s1 < 8 else s1) - 8
            for i in range(16):
                first[r, 32 * j + i] = 16 * s1 + i
                first[r, 32 * j + 16 + i] = 16 * s2 + i
            for i in range(32):
                skip[r, 32 * j + i] = 32 * sk + i
    return first, skip


def pick(table_row):
    want = jnp.tile(table_row.reshape(8, 1, 32), (1, 4, 1)).reshape(8, 128)
    want = want + (256 * (jnp.arange(128) // 32))[None, :]
    return (jnp.arange(1024)[:, None, None] == want[None]).astype(BF)


def edge_swap(face_lo, face_hi, d):
    send = jnp.where(d == 0, face_hi, face_lo)
    return lax.ppermute(send, "depth", [(0, 1), (1, 0)])


def row_halo(for_next, for_prev):
    lo = lax.ppermute(for_next, "row", [(i, i + 1) for i in range(15)])
    hi = lax.ppermute(for_prev, "row", [(i + 1, i) for i in range(15)])
    return lo, hi


def fine_halo(t, d):
    recv = edge_swap(t[:, 0], t[:, 7], d)
    t9 = jnp.concatenate([t, recv[:, None]], 1)
    lo, hi = row_halo(t9[1], t9[0])
    return jnp.stack([lo, t9[0], t9[1], hi])


def to_slab(t4, sel, d):
    rows = t4.reshape(4, 144, 256)
    sel = sel.reshape(4, 256, 8, 128)
    mixed = jnp.einsum("prc,pcjk->jrk", rows, sel, preferred_element_type=F32).astype(BF)
    got = lax.all_to_all(mixed, "col", 0, 0, tiled=True)
    planes = got.reshape(8, 9, 16, 128).transpose(1, 0, 2, 3).reshape(9, 128, 128)
    return z_ends(planes, d)


def z_ends(planes, d):
    last = planes[-1:]
    none = jnp.zeros_like(last)
    return jnp.concatenate([jnp.where(d == 0, none, last), planes[:-1], jnp.where(d == 0, last, none)], 0)


def slab_weights(w):
    w = w.reshape(3, 9, 32, 256)
    zero = jnp.zeros((1, 9, 32, 256), w.dtype)
    left = jnp.concatenate([w, zero], 0)
    right = jnp.concatenate([zero, w], 0)
    both = jnp.stack([left, right], 3)
    return both.transpose(1, 0, 2, 3, 4).reshape(9, 128, 512)


def slab_conv(planes, wt):
    pad = jnp.pad(planes, ((0, 0), (1, 1), (0, 0)))
    cols = [pad[c : c + 8, b : b + 128] for b in range(3) for c in range(3)]
    patches = jnp.concatenate(cols, -1).reshape(1024, 1152)
    return jnp.dot(patches, wt.reshape(1152, 512), preferred_element_type=F32)


def reduce_tiles(acc, j):
    y, c = j // 2, j % 2
    t = acc.reshape(8, 4, 2, 16, 512).transpose(2, 1, 0, 3, 4)
    keep = jnp.where(c == 0, t[0], t[1])
    send = jnp.where(c == 0, t[1], t[0])
    pair = keep + lax.ppermute(send, "col", [(i, i ^ 1) for i in range(8)])
    pair = jnp.roll(pair, -y, 0)
    total = pair[0]
    for o in (1, 3, 2):
        perm = [(2 * a + b, 2 * ((a + o) % 4) + b) for a in range(4) for b in range(2)]
        total = total + lax.ppermute(pair[o].astype(BF), "col", perm).astype(F32)
    return total


def body(volume, first_kernel, down_kernel, mid_kernel, up_kernel, last_kernel):
    r, j, d = (lax.axis_index(a) for a in ALL)
    p1, p2 = shard_perms()
    first_table, skip_table = (jnp.asarray(t) for t in tables())
    w1 = jnp.concatenate([lax.ppermute(first_kernel, ALL, p) for p in (p1, p2)], 1)
    la, lb = (lax.ppermute(last_kernel, ALL, p) for p in (p1, p2))
    in_low = (r // 4 + j % 2) % 4 < 2
    w_lift, w_skip = jnp.where(in_low, la, lb), jnp.where(in_low, lb, la)
    base = (jnp.where(in_low, 0, 2) + r // 4 + j % 2) % 4 * 4
    lift_at = base + (r % 4 + jnp.where(in_low, j // 2, -(j // 2))) % 4

    tile = volume.transpose(0, 2, 1, 3)
    planes = to_slab(fine_halo(tile, d), pick(first_table[r]), d)
    part = slab_conv(planes, slab_weights(w1))
    skip = jax.nn.gelu(reduce_tiles(part, j)).astype(BF).reshape(8, 16, 2, 256)

    cells = skip.reshape(4, 2, 8, 2, 2, 256)
    down = down_kernel.reshape(2, 2, 2, 256, 512)
    coarse = jax.nn.gelu(jnp.einsum("kcjbae,abceo->kjo", cells, down, preferred_element_type=F32)).astype(BF)
    recv = edge_swap(coarse[0], coarse[3], d)
    c5 = jnp.concatenate([coarse, recv[None]], 0)
    lo, hi = row_halo(c5, c5)
    c3 = jnp.stack([lo, c5, hi])
    got = lax.all_gather(c3, "col", axis=0)
    slab = got.transpose(1, 2, 0, 3, 4).reshape(3, 5, 64, 512)
    slab = jnp.stack([z_ends(slab[a], d) for a in range(3)])
    wm = mid_kernel.reshape(3, 3, 3, 512, 64).transpose(0, 2, 3, 1, 4).reshape(9, 512, 192)
    g = sum(
        jnp.dot(slab[a, c : c + 4].reshape(256, 512), wm[3 * a + c], preferred_element_type=F32)
        for a in range(3)
        for c in range(3)
    )
    g = jnp.pad(g.reshape(4, 64, 192), ((0, 0), (1, 1), (0, 0)))
    middle = jax.nn.gelu(g[:, 0:64, 0:64] + g[:, 1:65, 64:128] + g[:, 2:66, 128:192]).astype(BF)

    slab_skip = to_slab(fine_halo(skip.transpose(2, 0, 1, 3), d), pick(skip_table[r]), d)
    part = slab_conv(slab_skip, slab_weights(w_skip))

    recv = edge_swap(middle[0], middle[3], d)
    m5 = jnp.concatenate([middle, recv[None]], 0)
    lo, hi = row_halo(m5, m5)
    m3 = jnp.stack([lo, m5, hi])
    packed = jnp.concatenate([m3.reshape(15, 64, 64), jnp.zeros((1, 64, 64), BF)], 0)
    packed = packed.reshape(8, 2, 64, 64).transpose(0, 2, 1, 3).reshape(512, 128)
    got = lax.all_gather(packed, "col", axis=0)
    got = got.reshape(8, 8, 64, 2, 64).transpose(1, 3, 2, 0, 4).reshape(16, 64, 512)[:15].reshape(3, 5, 64, 512)
    up = lax.dynamic_slice(up_kernel, (0, 0, 32 * lift_at), (8, 512, 32)).reshape(2, 2, 2, 512, 32)
    rows = [
        jnp.einsum("kye,bceo->kcybo", got[m], up[a], preferred_element_type=F32).astype(BF)
        for m, a in ((0, 1), (1, 0), (1, 1), (2, 0))
    ]
    lift = jnp.stack(rows, -2).reshape(5, 2, 128, 128)
    own = lift[:4].reshape(8, 128, 128)
    end = jnp.where(d == 0, lift[4, 0], lift[4, 1])[None]
    planes = z_ends(jnp.concatenate([own, end], 0), d)
    part = part + slab_conv(planes, slab_weights(w_lift))
    out = jax.nn.gelu(reduce_tiles(part, j)).astype(BF).reshape(8, 16, 2, 256)
    return out.transpose(2, 1, 0, 3)


def solution(mesh):
    cells = P("row", "col", "depth", None)
    rows = P(None, "row", None)
    return jax.shard_map(
        body,
        mesh=mesh,
        in_specs=(cells, rows, P(), P(None, None, "col"), P(), rows),
        out_specs=cells,
        check_vma=False,
    )
```

```python
import jax
import jax.numpy as jnp
import numpy as np
from jax import lax
from jax.experimental import pallas as pl
from jax.experimental.pallas import tpu as pltpu
from jax.sharding import PartitionSpec as P

BF = jnp.bfloat16
F32 = jnp.float32
ALL = ("row", "col", "depth")


def shards_of(r, j):
    zhi, x = r // 4, r % 4
    y, c = j // 2, j % 2
    s1 = ((zhi + c) % 4) * 4 + (x + y) % 4
    s2 = ((zhi + c + 2) % 4) * 4 + (x - y) % 4
    return s1, s2


def flat(r, j, d):
    return (r * 8 + j) * 2 + d


def shard_perms():
    p1, p2 = [], []
    for r in range(16):
        for j in range(8):
            for d in range(2):
                s1, s2 = shards_of(r, j)
                p1.append((flat(s1, j, d), flat(r, j, d)))
                p2.append((flat(s2, j, d if j % 2 else 1 - d), flat(r, j, d)))
    return p1, p2


def tables():
    first = np.zeros((16, 256), np.int32)
    skip = np.zeros((16, 256), np.int32)
    for r in range(16):
        for j in range(8):
            s1, s2 = shards_of(r, j)
            sk = (s2 if s1 < 8 else s1) - 8
            for i in range(16):
                first[r, 32 * j + i] = 16 * s1 + i
                first[r, 32 * j + 16 + i] = 16 * s2 + i
            for i in range(32):
                skip[r, 32 * j + i] = 32 * sk + i
    return first, skip


def lift_table():
    places = np.zeros((16, 8), np.int32)
    for r in range(16):
        for j in range(8):
            places[r, j] = min(shards_of(r, j))
    return places


def pick(table_row):
    want = jnp.tile(table_row.reshape(8, 1, 32), (1, 4, 1)).reshape(8, 128)
    want = want + (256 * (jnp.arange(128) // 32))[None, :]
    return (jnp.arange(1024)[:, None, None] == want[None]).astype(BF)


def edge_swap(face_lo, face_hi, d):
    send = jnp.where(d == 0, face_hi, face_lo)
    return lax.ppermute(send, "depth", [(0, 1), (1, 0)])


def row_halo(for_next, for_prev):
    lo = lax.ppermute(for_next, "row", [(i, i + 1) for i in range(15)])
    hi = lax.ppermute(for_prev, "row", [(i + 1, i) for i in range(15)])
    return lo, hi


def fine_halo(t, d):
    recv = edge_swap(t[:, 0], t[:, 7], d)
    t9 = jnp.concatenate([t, recv[:, None]], 1)
    lo, hi = row_halo(t9[1], t9[0])
    return jnp.stack([lo, t9[0], t9[1], hi])


def to_slab(t4, sel, d):
    rows = t4.reshape(4, 144, 256)
    sel = sel.reshape(4, 256, 8, 128)
    mixed = jnp.einsum("prc,pcjk->jrk", rows, sel, preferred_element_type=F32).astype(BF)
    got = lax.all_to_all(mixed, "col", 0, 0, tiled=True)
    planes = got.reshape(8, 9, 16, 128).transpose(1, 0, 2, 3).reshape(9, 128, 128)
    return z_ends(planes, d)


def z_ends(planes, d):
    last = planes[-1:]
    none = jnp.zeros_like(last)
    return jnp.concatenate([jnp.where(d == 0, none, last), planes[:-1], jnp.where(d == 0, last, none)], 0)


def slab_weights(w):
    w = w.reshape(3, 9, 32, 256)
    zero = jnp.zeros((1, 9, 32, 256), w.dtype)
    left = jnp.concatenate([w, zero], 0)
    right = jnp.concatenate([zero, w], 0)
    both = jnp.stack([left, right], 3)
    return both.transpose(1, 0, 2, 3, 4).reshape(9, 128, 512)


def slab_conv(planes, wt):
    pad = jnp.pad(planes, ((0, 0), (1, 1), (0, 0)))
    cols = [pad[c : c + 8, b : b + 128] for b in range(3) for c in range(3)]
    patches = jnp.concatenate(cols, -1).reshape(1024, 1152)
    return jnp.dot(patches, wt.reshape(1152, 512), preferred_element_type=F32)


def mid_body(slab_ref, w_ref, prev_ref, own_ref, next_ref):
    y = lax.broadcasted_iota(jnp.int32, (320, 64), 0) % 64
    near = [slab_ref[c : c + 5].reshape(320, 512) for c in range(3)]
    for a, out in enumerate((prev_ref, own_ref, next_ref)):
        total = jnp.zeros((320, 64), F32)
        for b in range(3):
            g = jnp.zeros((320, 64), F32)
            for c in range(3):
                g = g + jnp.dot(near[c], w_ref[9 * a + 3 * b + c], preferred_element_type=F32)
            if b == 0:
                g = jnp.where(y == 0, 0.0, pltpu.roll(g, 1, 0))
            if b == 2:
                g = jnp.where(y == 63, 0.0, pltpu.roll(g, 319, 0))
            total = total + g
        out[...] = total.reshape(5, 64, 64).astype(out.dtype)


def mid_taps(slab, w):
    whole = pl.BlockSpec(memory_space=pltpu.VMEM)
    return pl.pallas_call(
        mid_body,
        in_specs=[whole] * 2,
        out_specs=[whole] * 3,
        out_shape=[jax.ShapeDtypeStruct((5, 64, 64), t) for t in (BF, F32, BF)],
        compiler_params=pltpu.CompilerParams(vmem_limit_bytes=24 << 20),
        name="mid_taps",
    )(slab, w)


def reduce_tiles(acc, j):
    y, c = j // 2, j % 2
    t = acc.reshape(8, 4, 2, 16, 512).transpose(2, 1, 0, 3, 4)
    keep = jnp.where(c == 0, t[0], t[1])
    send = jnp.where(c == 0, t[1], t[0])
    pair = keep + lax.ppermute(send, "col", [(i, i ^ 1) for i in range(8)])
    pair = jnp.roll(pair, -y, 0)
    total = pair[0]
    for o in (1, 3, 2):
        perm = [(2 * a + b, 2 * ((a + o) % 4) + b) for a in range(4) for b in range(2)]
        total = total + lax.ppermute(pair[o].astype(BF), "col", perm).astype(F32)
    return total


def body(volume, first_kernel, down_kernel, mid_kernel, up_kernel, last_kernel):
    r, j, d = (lax.axis_index(a) for a in ALL)
    p1, p2 = shard_perms()
    first_table, skip_table = (jnp.asarray(t) for t in tables())
    w1 = jnp.concatenate([lax.ppermute(first_kernel, ALL, p) for p in (p1, p2)], 1)
    in_low = (r // 4 + j % 2) % 4 < 2

    tile = volume.transpose(0, 2, 1, 3)
    t4, w1, last_kernel = lax.optimization_barrier((fine_halo(tile, d), w1, last_kernel))
    la = lax.ppermute(last_kernel, ALL, p1)
    lb = lax.ppermute(last_kernel, ALL, p2)
    planes = to_slab(t4, pick(first_table[r]), d)
    part = slab_conv(planes, slab_weights(w1))
    skip = jax.nn.gelu(reduce_tiles(part, j)).astype(BF).reshape(8, 16, 2, 256)

    cells = skip.reshape(4, 2, 8, 2, 2, 256)
    down = down_kernel.reshape(2, 2, 2, 256, 512)
    coarse = jax.nn.gelu(jnp.einsum("kcjbae,abceo->kjo", cells, down, preferred_element_type=F32)).astype(BF)
    send = jnp.where(d == 0, coarse[2:], coarse[:2])
    recv = lax.ppermute(send, "depth", [(0, 1), (1, 0)])
    got = lax.all_gather(jnp.concatenate([coarse, recv], 0), "col", axis=0)
    got = got.transpose(1, 0, 2, 3).reshape(6, 64, 512)
    none = jnp.zeros((1, 64, 512), BF)
    slab = jnp.where(
        d == 0, jnp.concatenate([none, got], 0), jnp.concatenate([got[4:], got[:4], none], 0)
    )
    h = mid_taps(slab, mid_kernel)
    lo, hi = row_halo(h[0], h[2])
    middle = jax.nn.gelu(h[1] + lo.astype(F32) + hi.astype(F32)).astype(BF)

    slab_skip = to_slab(fine_halo(skip.transpose(2, 0, 1, 3), d), pick(skip_table[r]), d)

    middle, la, lb, slab_skip = lax.optimization_barrier((middle, la, lb, slab_skip))
    w_lift, w_skip = jnp.where(in_low, la, lb), jnp.where(in_low, lb, la)
    part = slab_conv(slab_skip, slab_weights(w_skip))

    packed = jnp.concatenate([middle, jnp.zeros((1, 64, 64), BF)], 0)
    packed = packed.reshape(3, 2, 64, 64).transpose(0, 2, 1, 3).reshape(3, 64, 128)
    got = lax.all_gather(packed, "col", axis=0)
    got = got.transpose(1, 2, 0, 3).reshape(192, 1024)
    places = jnp.asarray(lift_table())

    def cut(row):
        at = places[jnp.clip(row, 0, 15), j]
        return lax.dynamic_slice(up_kernel, (0, 0, 32 * at), (8, 512, 32)).reshape(2, 2, 2, 8, 64, 32)

    mine = cut(r)
    up = jnp.stack([cut(r - 1)[0], mine[0], mine[1], cut(r + 1)[1]])
    up = up.transpose(3, 4, 1, 2, 0, 5).reshape(8, 64, 2, 2, 128)
    zero = jnp.zeros_like(up)
    up = jnp.stack([jnp.stack([up, zero], 2), jnp.stack([zero, up], 2)], 1)
    lift = jnp.dot(got, up.reshape(1024, 1024), preferred_element_type=F32).astype(BF)
    lift = lift.reshape(3, 64, 2, 2, 2, 128).transpose(0, 2, 4, 1, 3, 5).reshape(12, 128, 128)
    none = jnp.zeros((1, 128, 128), BF)
    lift = jnp.where(d == 0, jnp.concatenate([none, lift[:9]], 0), jnp.concatenate([lift[1:10], none], 0))

    def pack(v):
        v = jnp.concatenate([v, jnp.zeros((2, 128, 32), BF)], 0)
        return v.reshape(3, 4, 128, 32).transpose(0, 2, 1, 3).reshape(3, 128, 128)

    def unpack(v):
        return v.reshape(3, 128, 4, 32).transpose(0, 2, 1, 3).reshape(12, 128, 32)[:10]

    lo, hi = row_halo(pack(lift[..., 96:]), pack(lift[..., :32]))
    planes = jnp.concatenate([unpack(lo), lift[..., 32:96], unpack(hi)], -1)
    part = part + slab_conv(planes, slab_weights(w_lift))
    out = jax.nn.gelu(reduce_tiles(part, j)).astype(BF).reshape(8, 16, 2, 256)
    return out.transpose(2, 1, 0, 3)


def solution(mesh):
    cells = P("row", "col", "depth", None)
    rows = P(None, "row", None)
    return jax.shard_map(
        body,
        mesh=mesh,
        in_specs=(cells, rows, P(), P(None, None, "col"), P(), rows),
        out_specs=cells,
        check_vma=False,
    )
```

```python
import jax
import jax.numpy as jnp
import numpy as np
from jax import lax
from jax.experimental import pallas as pl
from jax.experimental.pallas import tpu as pltpu
from jax.sharding import PartitionSpec as P

BF = jnp.bfloat16
F32 = jnp.float32
ALL = ("row", "col", "depth")


def shards_of(r, j):
    zhi, x = r // 4, r % 4
    y, c = j // 2, j % 2
    s1 = ((zhi + c) % 4) * 4 + (x + y) % 4
    s2 = ((zhi + c + 2) % 4) * 4 + (x - y) % 4
    return s1, s2


def flat(r, j, d):
    return (r * 8 + j) * 2 + d


def shard_perms():
    p1, p2 = [], []
    for r in range(16):
        for j in range(8):
            for d in range(2):
                s1, s2 = shards_of(r, j)
                p1.append((flat(s1, j, d), flat(r, j, d)))
                p2.append((flat(s2, j, d if j % 2 else 1 - d), flat(r, j, d)))
    return p1, p2


def tables():
    first = np.zeros((16, 256), np.int32)
    skip = np.zeros((16, 256), np.int32)
    for r in range(16):
        for j in range(8):
            s1, s2 = shards_of(r, j)
            sk = (s2 if s1 < 8 else s1) - 8
            for i in range(16):
                first[r, 32 * j + i] = 16 * s1 + i
                first[r, 32 * j + 16 + i] = 16 * s2 + i
            for i in range(32):
                skip[r, 32 * j + i] = 32 * sk + i
    return first, skip


def lift_table():
    places = np.zeros((16, 8), np.int32)
    for r in range(16):
        for j in range(8):
            places[r, j] = min(shards_of(r, j))
    return places


def pick(table_row):
    want = jnp.tile(table_row.reshape(8, 1, 32), (1, 4, 1)).reshape(8, 128)
    want = want + (256 * (jnp.arange(128) // 32))[None, :]
    return (jnp.arange(1024)[:, None, None] == want[None]).astype(BF)


def edge_swap(face_lo, face_hi, d):
    send = jnp.where(d == 0, face_hi, face_lo)
    return lax.ppermute(send, "depth", [(0, 1), (1, 0)])


def row_halo(for_next, for_prev):
    lo = lax.ppermute(for_next, "row", [(i, i + 1) for i in range(15)])
    hi = lax.ppermute(for_prev, "row", [(i + 1, i) for i in range(15)])
    return lo, hi


def fine_halo(t, d):
    recv = edge_swap(t[:, 0], t[:, 7], d)
    t9 = jnp.concatenate([t, recv[:, None]], 1)
    lo, hi = row_halo(t9[1], t9[0])
    return jnp.stack([lo, t9[0], t9[1], hi])


def to_slab(t4, sel, d):
    rows = t4.reshape(4, 144, 256)
    sel = sel.reshape(4, 256, 8, 128)
    mixed = jnp.einsum("prc,pcjk->jrk", rows, sel, preferred_element_type=F32).astype(BF)
    got = lax.all_to_all(mixed, "col", 0, 0, tiled=True)
    planes = got.reshape(8, 9, 16, 128).transpose(1, 0, 2, 3).reshape(9, 128, 128)
    return z_ends(planes, d)


def z_ends(planes, d):
    last = planes[-1:]
    none = jnp.zeros_like(last)
    return jnp.concatenate([jnp.where(d == 0, none, last), planes[:-1], jnp.where(d == 0, last, none)], 0)


def slab_weights(w):
    w = w.reshape(3, 9, 32, 256)
    zero = jnp.zeros((1, 9, 32, 256), w.dtype)
    left = jnp.concatenate([w, zero], 0)
    right = jnp.concatenate([zero, w], 0)
    both = jnp.stack([left, right], 3)
    return both.transpose(1, 0, 2, 3, 4).reshape(9, 128, 512)


def slab_conv(planes, wt):
    pad = jnp.pad(planes, ((0, 0), (1, 1), (0, 0)))
    cols = [pad[c : c + 8, b : b + 128] for b in range(3) for c in range(3)]
    patches = jnp.concatenate(cols, -1).reshape(1024, 1152)
    return jnp.dot(patches, wt.reshape(1152, 512), preferred_element_type=F32)


WHOLE = pl.BlockSpec(memory_space=pltpu.VMEM)


def mid_body(slab_ref, w_hbm, prev_ref, own_ref, next_ref, w_ref, sems):
    copies = [
        pltpu.make_async_copy(w_hbm.at[pl.ds(9 * a, 9)], w_ref.at[pl.ds(9 * a, 9)], sems.at[a]) for a in range(3)
    ]
    for copy in copies:
        copy.start()
    y = lax.broadcasted_iota(jnp.int32, (320, 64), 0) % 64
    near = [slab_ref[c : c + 5].reshape(320, 512) for c in range(3)]
    for a, out in enumerate((prev_ref, own_ref, next_ref)):
        copies[a].wait()
        total = jnp.zeros((320, 64), F32)
        for b in range(3):
            g = jnp.zeros((320, 64), F32)
            for c in range(3):
                g = g + jnp.dot(near[c], w_ref[9 * a + 3 * b + c], preferred_element_type=F32)
            if b == 0:
                g = jnp.where(y == 0, 0.0, pltpu.roll(g, 1, 0))
            if b == 2:
                g = jnp.where(y == 63, 0.0, pltpu.roll(g, 319, 0))
            total = total + g
        out[...] = total.reshape(5, 64, 64).astype(out.dtype)


def mid_taps(slab, w):
    return pl.pallas_call(
        mid_body,
        in_specs=[WHOLE, pl.BlockSpec(memory_space=pl.ANY)],
        out_specs=[WHOLE] * 3,
        out_shape=[jax.ShapeDtypeStruct((5, 64, 64), t) for t in (BF, F32, BF)],
        scratch_shapes=[pltpu.VMEM((27, 512, 64), BF), pltpu.SemaphoreType.DMA((3,))],
        compiler_params=pltpu.CompilerParams(vmem_limit_bytes=24 << 20),
        name="mid_taps",
    )(slab, w)


def lift_body(at_ref, got_ref, up_ref, planes_ref, next_ref, prev_ref, w_ref, tmp_ref):
    w_ref[...] = jnp.zeros((1024, 1024), BF)
    ch = lax.broadcasted_iota(jnp.int32, (256, 128), 0)
    lane = lax.broadcasted_iota(jnp.int32, (256, 128), 1)
    part, within = lane // 32, lane % 32
    shard = jnp.where(part == 0, at_ref[0], jnp.where(part == 3, at_ref[2], at_ref[1]))
    hit = ch == 32 * shard + within
    upper = jnp.where(hit & (part < 2), 1.0, 0.0).astype(BF)
    lower = jnp.where(hit & (part >= 2), 1.0, 0.0).astype(BF)
    for tap in range(4):
        u = jnp.dot(up_ref[tap], upper, preferred_element_type=F32)
        u = u + jnp.dot(up_ref[4 + tap], lower, preferred_element_type=F32)
        u = u.astype(BF)
        for src in range(8):
            for h in range(2):
                rows = slice(128 * src + 64 * h, 128 * src + 64 * h + 64)
                w_ref[rows, 128 * (4 * h + tap) : 128 * (4 * h + tap) + 128] = u[64 * src : 64 * src + 64]
    got = jnp.concatenate(
        [jnp.concatenate([got_ref[src, g] for src in range(8)], 1) for g in range(3)], 0
    )
    out = jnp.dot(got, w_ref[...], preferred_element_type=F32)
    for g in range(3):
        for h in range(2):
            for b in range(2):
                for c in range(2):
                    piece = out[64 * g : 64 * g + 64, 128 * (4 * h + 2 * b + c) : 128 * (4 * h + 2 * b + c) + 128]
                    tmp_ref[2 * (2 * g + h) + c, pl.ds(b, 64, stride=2), :] = piece
    group = lax.broadcasted_iota(jnp.int32, (128, 128), 1) // 32
    for q in range(3):
        nxt = jnp.zeros((128, 128), F32)
        prv = jnp.zeros((128, 128), F32)
        for k in range(4):
            plane = tmp_ref[4 * q + k]
            planes_ref[4 * q + k] = plane.astype(BF)
            nxt = jnp.where(group == k, pltpu.roll(plane, (32 * k - 96) % 128, 1), nxt)
            prv = jnp.where(group == k, pltpu.roll(plane, 32 * k, 1) if k else plane, prv)
        next_ref[q] = nxt.astype(BF)
        prev_ref[q] = prv.astype(BF)


def lift_planes(at, got, up):
    return pl.pallas_call(
        lift_body,
        in_specs=[pl.BlockSpec(memory_space=pltpu.SMEM), WHOLE, WHOLE],
        out_specs=[WHOLE] * 3,
        out_shape=[jax.ShapeDtypeStruct((n, 128, 128), BF) for n in (12, 3, 3)],
        scratch_shapes=[pltpu.VMEM((1024, 1024), BF), pltpu.VMEM((12, 128, 128), F32)],
        compiler_params=pltpu.CompilerParams(vmem_limit_bytes=24 << 20),
        name="lift_planes",
    )(at, got, up)


def reduce_tiles(acc, j):
    y, c = j // 2, j % 2
    t = acc.reshape(8, 4, 2, 16, 512).transpose(2, 1, 0, 3, 4)
    keep = jnp.where(c == 0, t[0], t[1])
    send = jnp.where(c == 0, t[1], t[0])
    pair = keep + lax.ppermute(send, "col", [(i, i ^ 1) for i in range(8)])
    pair = jnp.roll(pair, -y, 0)
    total = pair[0]
    for o in (1, 3, 2):
        perm = [(2 * a + b, 2 * ((a + o) % 4) + b) for a in range(4) for b in range(2)]
        total = total + lax.ppermute(pair[o].astype(BF), "col", perm).astype(F32)
    return total


def body(volume, first_kernel, down_kernel, mid_kernel, up_kernel, last_kernel):
    r, j, d = (lax.axis_index(a) for a in ALL)
    p1, p2 = shard_perms()
    first_table, skip_table = (jnp.asarray(t) for t in tables())
    w1 = jnp.concatenate([lax.ppermute(first_kernel, ALL, p) for p in (p1, p2)], 1)
    in_low = (r // 4 + j % 2) % 4 < 2

    tile = volume.transpose(0, 2, 1, 3)
    t4, w1, last_kernel = lax.optimization_barrier((fine_halo(tile, d), w1, last_kernel))
    la = lax.ppermute(last_kernel, ALL, p1)
    lb = lax.ppermute(last_kernel, ALL, p2)
    planes = to_slab(t4, pick(first_table[r]), d)
    part = slab_conv(planes, slab_weights(w1))
    skip = jax.nn.gelu(reduce_tiles(part, j)).astype(BF).reshape(8, 16, 2, 256)

    cells = skip.reshape(4, 2, 8, 2, 2, 256)
    down = down_kernel.reshape(2, 2, 2, 256, 512)
    coarse = jax.nn.gelu(jnp.einsum("kcjbae,abceo->kjo", cells, down, preferred_element_type=F32)).astype(BF)
    send = jnp.where(d == 0, coarse[2:], coarse[:2])
    recv = lax.ppermute(send, "depth", [(0, 1), (1, 0)])
    got = lax.all_gather(jnp.concatenate([coarse, recv], 0), "col", axis=0)
    got = got.transpose(1, 0, 2, 3).reshape(6, 64, 512)
    none = jnp.zeros((1, 64, 512), BF)
    slab = jnp.where(
        d == 0, jnp.concatenate([none, got], 0), jnp.concatenate([got[4:], got[:4], none], 0)
    )
    h = mid_taps(slab, mid_kernel)
    lo, hi = row_halo(h[0], h[2])
    middle = jax.nn.gelu(h[1] + lo.astype(F32) + hi.astype(F32)).astype(BF)

    slab_skip = to_slab(fine_halo(skip.transpose(2, 0, 1, 3), d), pick(skip_table[r]), d)

    middle, la, lb, slab_skip = lax.optimization_barrier((middle, la, lb, slab_skip))
    w_lift, w_skip = jnp.where(in_low, la, lb), jnp.where(in_low, lb, la)
    part = slab_conv(slab_skip, slab_weights(w_skip))

    packed = jnp.concatenate([middle, jnp.zeros((1, 64, 64), BF)], 0)
    packed = packed.reshape(3, 2, 64, 64).transpose(0, 2, 1, 3).reshape(3, 64, 128)
    got = lax.all_gather(packed, "col", axis=0)
    places = jnp.asarray(lift_table())
    at = jnp.stack([places[jnp.clip(r + step, 0, 15), j] for step in (-1, 0, 1)])
    lift, for_next, for_prev = lift_planes(at, got, up_kernel)

    def unpack(v):
        return v.reshape(3, 128, 4, 32).transpose(0, 2, 1, 3).reshape(12, 128, 32)

    lo, hi = row_halo(for_next, for_prev)
    lift = jnp.concatenate([unpack(lo), lift[..., 32:96], unpack(hi)], -1)
    none = jnp.zeros((1, 128, 128), BF)
    planes = jnp.where(d == 0, jnp.concatenate([none, lift[:9]], 0), jnp.concatenate([lift[1:10], none], 0))
    part = part + slab_conv(planes, slab_weights(w_lift))
    out = jax.nn.gelu(reduce_tiles(part, j)).astype(BF).reshape(8, 16, 2, 256)
    return out.transpose(2, 1, 0, 3)


def solution(mesh):
    cells = P("row", "col", "depth", None)
    rows = P(None, "row", None)
    return jax.shard_map(
        body,
        mesh=mesh,
        in_specs=(cells, rows, P(), P(None, None, "col"), P(), rows),
        out_specs=cells,
        check_vma=False,
    )
```

```python
import jax
import jax.numpy as jnp
import numpy as np
from jax import lax
from jax.experimental import pallas as pl
from jax.experimental.pallas import tpu as pltpu
from jax.sharding import PartitionSpec as P

BF = jnp.bfloat16
F32 = jnp.float32
ALL = ("row", "col", "depth")


def shards_of(r, j):
    zhi, x = r // 4, r % 4
    y, c = j // 2, j % 2
    s1 = ((zhi + c) % 4) * 4 + (x + y) % 4
    s2 = ((zhi + c + 2) % 4) * 4 + (x - y) % 4
    return s1, s2


def flat(r, j, d):
    return (r * 8 + j) * 2 + d


def shard_perms():
    p1, p2 = [], []
    for r in range(16):
        for j in range(8):
            for d in range(2):
                s1, s2 = shards_of(r, j)
                p1.append((flat(s1, j, d), flat(r, j, d)))
                p2.append((flat(s2, j, d if j % 2 else 1 - d), flat(r, j, d)))
    return p1, p2


def tables():
    first = np.zeros((16, 256), np.int32)
    skip = np.zeros((16, 256), np.int32)
    for r in range(16):
        for j in range(8):
            s1, s2 = shards_of(r, j)
            sk = (s2 if s1 < 8 else s1) - 8
            for i in range(16):
                first[r, 32 * j + i] = 16 * s1 + i
                first[r, 32 * j + 16 + i] = 16 * s2 + i
            for i in range(32):
                skip[r, 32 * j + i] = 32 * sk + i
    return first, skip


def lift_table():
    places = np.zeros((16, 8), np.int32)
    for r in range(16):
        for j in range(8):
            places[r, j] = min(shards_of(r, j))
    return places


def pick(table_row):
    want = jnp.tile(table_row.reshape(8, 1, 32), (1, 4, 1)).reshape(8, 128)
    want = want + (256 * (jnp.arange(128) // 32))[None, :]
    return (jnp.arange(1024)[:, None, None] == want[None]).astype(BF)


def edge_swap(face_lo, face_hi, d):
    send = jnp.where(d == 0, face_hi, face_lo)
    return lax.ppermute(send, "depth", [(0, 1), (1, 0)])


def row_halo(for_next, for_prev):
    lo = lax.ppermute(for_next, "row", [(i, i + 1) for i in range(15)])
    hi = lax.ppermute(for_prev, "row", [(i + 1, i) for i in range(15)])
    return lo, hi


def fine_halo(t, d):
    recv = edge_swap(t[:, 0], t[:, 7], d)
    t9 = jnp.concatenate([t, recv[:, None]], 1)
    lo, hi = row_halo(t9[1], t9[0])
    return jnp.stack([lo, t9[0], t9[1], hi])


def to_slab(t4, sel):
    rows = t4.reshape(4, 144, 256)
    sel = sel.reshape(4, 256, 8, 128)
    mixed = jnp.einsum("prc,pcjk->jrk", rows, sel, preferred_element_type=F32).astype(BF)
    got = lax.all_to_all(mixed, "col", 0, 0, tiled=True)
    return got


WHOLE = pl.BlockSpec(memory_space=pltpu.VMEM)
SCALARS = pl.BlockSpec(memory_space=pltpu.SMEM)


def fill_weights(tap, wt_ref):
    none = jnp.zeros((32, 256), BF)
    for blk in range(9):
        for p in range(4):
            for xo in range(2):
                rows = slice(128 * blk + 32 * p, 128 * blk + 32 * p + 32)
                value = tap(9 * (p - xo) + blk) if 0 <= p - xo <= 2 else none
                wt_ref[rows, 256 * xo : 256 * xo + 256] = value


def fill_plane(q, plane, patch_ref):
    y = lax.broadcasted_iota(jnp.int32, (128, 128), 0)
    shifted = (
        jnp.where(y == 0, 0.0, pltpu.roll(plane, 1, 0)),
        plane,
        jnp.where(y == 127, 0.0, pltpu.roll(plane, 127, 0)),
    )
    for b in range(3):
        value = shifted[b].astype(BF)
        for c in range(3):
            if 0 <= q - c < 8:
                rows = slice(128 * (q - c), 128 * (q - c) + 128)
                patch_ref[rows, 128 * (3 * b + c) : 128 * (3 * b + c) + 128] = value


def fill_from_exchange(d, got_ref, patch_ref):
    for z in range(9):
        plane = jnp.concatenate([got_ref[src, 16 * z : 16 * z + 16].astype(F32) for src in range(8)], 0)
        if z < 8:
            fill_plane(z + 1, plane, patch_ref)
        else:
            fill_plane(0, jnp.where(d == 1, plane, 0.0), patch_ref)
            fill_plane(9, jnp.where(d == 0, plane, 0.0), patch_ref)


def split_tiles(core, acc, keep_ref, send_ref):
    acc = acc.reshape(8, 128, 512)
    for y in range(4):
        first, second = acc[:, 32 * y : 32 * y + 16], acc[:, 32 * y + 16 : 32 * y + 32]
        keep_ref[y] = jnp.where(core == 0, first, second)
        send_ref[y] = jnp.where(core == 0, second, first)


def first_body(at_ref, got_ref, wa_ref, wb_ref, keep_ref, send_ref, wt_ref, patch_ref):
    fill_weights(lambda n: jnp.concatenate([wa_ref[n], wb_ref[n]], 0), wt_ref)
    fill_from_exchange(at_ref[0], got_ref, patch_ref)
    acc = jnp.dot(patch_ref[...], wt_ref[...], preferred_element_type=F32)
    split_tiles(at_ref[1], acc, keep_ref, send_ref)


def skip_body(at_ref, got_ref, wa_ref, wb_ref, acc_ref, wt_ref, patch_ref):
    low = at_ref[2] == 1
    fill_weights(lambda n: jnp.where(low, wb_ref[n], wa_ref[n]), wt_ref)
    fill_from_exchange(at_ref[0], got_ref, patch_ref)
    acc_ref[...] = jnp.dot(patch_ref[...], wt_ref[...], preferred_element_type=F32)


def last_body(
    at_ref, lift_ref, lo_ref, hi_ref, wa_ref, wb_ref, part_ref, keep_ref, send_ref, wt_ref, patch_ref, full_ref
):
    low = at_ref[2] == 1
    d = at_ref[0]
    fill_weights(lambda n: jnp.where(low, wa_ref[n], wb_ref[n]), wt_ref)
    group = lax.broadcasted_iota(jnp.int32, (128, 128), 1) // 32
    for g in range(3):
        lo, hi = lo_ref[g].astype(F32), hi_ref[g].astype(F32)
        for k in range(4):
            plane = lift_ref[4 * g + k].astype(F32)
            left = pltpu.roll(lo, 128 - 32 * k, 1) if k else lo
            right = pltpu.roll(hi, 96 - 32 * k, 1) if k < 3 else hi
            full_ref[4 * g + k] = jnp.where(group == 0, left, jnp.where(group == 3, right, plane))
    for q in range(1, 9):
        fill_plane(q, full_ref[q - 1 + 2 * d], patch_ref)
    fill_plane(0, jnp.where(d == 1, full_ref[1], 0.0), patch_ref)
    fill_plane(9, jnp.where(d == 0, full_ref[8], 0.0), patch_ref)
    acc = part_ref[...] + jnp.dot(patch_ref[...], wt_ref[...], preferred_element_type=F32)
    split_tiles(at_ref[1], acc, keep_ref, send_ref)


def slab_call(kernel, at, *arrays, split=True, full=False):
    tiles = jax.ShapeDtypeStruct((4, 8, 16, 512), F32)
    return pl.pallas_call(
        kernel,
        in_specs=[SCALARS] + [WHOLE] * len(arrays),
        out_specs=[WHOLE] * 2 if split else WHOLE,
        out_shape=[tiles] * 2 if split else jax.ShapeDtypeStruct((1024, 512), F32),
        scratch_shapes=[pltpu.VMEM((1152, 512), BF), pltpu.VMEM((1024, 1152), BF)]
        + [pltpu.VMEM((12, 128, 128), F32)] * full,
        compiler_params=pltpu.CompilerParams(vmem_limit_bytes=32 << 20),
    )(at, *arrays)


def mid_body(slab_ref, w_hbm, prev_ref, own_ref, next_ref, w_ref, sems):
    copies = [
        pltpu.make_async_copy(w_hbm.at[pl.ds(9 * a, 9)], w_ref.at[pl.ds(9 * a, 9)], sems.at[a]) for a in range(3)
    ]
    for copy in copies:
        copy.start()
    y = lax.broadcasted_iota(jnp.int32, (320, 64), 0) % 64
    near = [slab_ref[c : c + 5].reshape(320, 512) for c in range(3)]
    for a, out in enumerate((prev_ref, own_ref, next_ref)):
        copies[a].wait()
        total = jnp.zeros((320, 64), F32)
        for b in range(3):
            g = jnp.zeros((320, 64), F32)
            for c in range(3):
                g = g + jnp.dot(near[c], w_ref[9 * a + 3 * b + c], preferred_element_type=F32)
            if b == 0:
                g = jnp.where(y == 0, 0.0, pltpu.roll(g, 1, 0))
            if b == 2:
                g = jnp.where(y == 63, 0.0, pltpu.roll(g, 319, 0))
            total = total + g
        out[...] = total.reshape(5, 64, 64).astype(out.dtype)


def mid_taps(slab, w):
    return pl.pallas_call(
        mid_body,
        in_specs=[WHOLE, pl.BlockSpec(memory_space=pl.ANY)],
        out_specs=[WHOLE] * 3,
        out_shape=[jax.ShapeDtypeStruct((5, 64, 64), t) for t in (BF, F32, BF)],
        scratch_shapes=[pltpu.VMEM((27, 512, 64), BF), pltpu.SemaphoreType.DMA((3,))],
        compiler_params=pltpu.CompilerParams(vmem_limit_bytes=24 << 20),
        name="mid_taps",
    )(slab, w)


def lift_body(at_ref, got_ref, up_ref, planes_ref, next_ref, prev_ref, w_ref, tmp_ref):
    w_ref[...] = jnp.zeros((1024, 1024), BF)
    ch = lax.broadcasted_iota(jnp.int32, (256, 128), 0)
    lane = lax.broadcasted_iota(jnp.int32, (256, 128), 1)
    part, within = lane // 32, lane % 32
    shard = jnp.where(part == 0, at_ref[0], jnp.where(part == 3, at_ref[2], at_ref[1]))
    hit = ch == 32 * shard + within
    upper = jnp.where(hit & (part < 2), 1.0, 0.0).astype(BF)
    lower = jnp.where(hit & (part >= 2), 1.0, 0.0).astype(BF)
    for tap in range(4):
        u = jnp.dot(up_ref[tap], upper, preferred_element_type=F32)
        u = u + jnp.dot(up_ref[4 + tap], lower, preferred_element_type=F32)
        u = u.astype(BF)
        for src in range(8):
            for h in range(2):
                rows = slice(128 * src + 64 * h, 128 * src + 64 * h + 64)
                w_ref[rows, 128 * (4 * h + tap) : 128 * (4 * h + tap) + 128] = u[64 * src : 64 * src + 64]
    got = jnp.concatenate(
        [jnp.concatenate([got_ref[src, g] for src in range(8)], 1) for g in range(3)], 0
    )
    out = jnp.dot(got, w_ref[...], preferred_element_type=F32)
    for g in range(3):
        for h in range(2):
            for b in range(2):
                for c in range(2):
                    piece = out[64 * g : 64 * g + 64, 128 * (4 * h + 2 * b + c) : 128 * (4 * h + 2 * b + c) + 128]
                    tmp_ref[2 * (2 * g + h) + c, pl.ds(b, 64, stride=2), :] = piece
    group = lax.broadcasted_iota(jnp.int32, (128, 128), 1) // 32
    for q in range(3):
        nxt = jnp.zeros((128, 128), F32)
        prv = jnp.zeros((128, 128), F32)
        for k in range(4):
            plane = tmp_ref[4 * q + k]
            planes_ref[4 * q + k] = plane.astype(BF)
            nxt = jnp.where(group == k, pltpu.roll(plane, (32 * k - 96) % 128, 1), nxt)
            prv = jnp.where(group == k, pltpu.roll(plane, 32 * k, 1) if k else plane, prv)
        next_ref[q] = nxt.astype(BF)
        prev_ref[q] = prv.astype(BF)


def lift_planes(at, got, up):
    return pl.pallas_call(
        lift_body,
        in_specs=[SCALARS, WHOLE, WHOLE],
        out_specs=[WHOLE] * 3,
        out_shape=[jax.ShapeDtypeStruct((n, 128, 128), BF) for n in (12, 3, 3)],
        scratch_shapes=[pltpu.VMEM((1024, 1024), BF), pltpu.VMEM((12, 128, 128), F32)],
        compiler_params=pltpu.CompilerParams(vmem_limit_bytes=24 << 20),
        name="lift_planes",
    )(at, got, up)


def reduce_tiles(keep, send, j):
    y = j // 2
    pair = keep + lax.ppermute(send, "col", [(i, i ^ 1) for i in range(8)])
    pair = jnp.roll(pair, -y, 0)
    total = pair[0]
    for o in (1, 3, 2):
        perm = [(2 * a + b, 2 * ((a + o) % 4) + b) for a in range(4) for b in range(2)]
        total = total + lax.ppermute(pair[o].astype(BF), "col", perm).astype(F32)
    return total


def body(volume, first_kernel, down_kernel, mid_kernel, up_kernel, last_kernel):
    r, j, d = (lax.axis_index(a) for a in ALL)
    p1, p2 = shard_perms()
    first_table, skip_table = (jnp.asarray(t) for t in tables())
    wa, wb = (lax.ppermute(first_kernel, ALL, p) for p in (p1, p2))
    in_low = (r // 4 + j % 2) % 4 < 2

    tile = volume.transpose(0, 2, 1, 3)
    t4, wa, wb, last_kernel = lax.optimization_barrier((fine_halo(tile, d), wa, wb, last_kernel))
    la = lax.ppermute(last_kernel, ALL, p1)
    lb = lax.ppermute(last_kernel, ALL, p2)
    at = jnp.stack([d, j % 2, in_low.astype(jnp.int32)])
    got = to_slab(t4, pick(first_table[r]))
    keep, send = slab_call(first_body, at, got, wa, wb)
    skip = jax.nn.gelu(reduce_tiles(keep, send, j)).astype(BF).reshape(8, 16, 2, 256)

    cells = skip.reshape(4, 2, 8, 2, 2, 256)
    down = down_kernel.reshape(2, 2, 2, 256, 512)
    coarse = jax.nn.gelu(jnp.einsum("kcjbae,abceo->kjo", cells, down, preferred_element_type=F32)).astype(BF)
    send = jnp.where(d == 0, coarse[2:], coarse[:2])
    recv = lax.ppermute(send, "depth", [(0, 1), (1, 0)])
    got = lax.all_gather(jnp.concatenate([coarse, recv], 0), "col", axis=0)
    got = got.transpose(1, 0, 2, 3).reshape(6, 64, 512)
    none = jnp.zeros((1, 64, 512), BF)
    slab = jnp.where(
        d == 0, jnp.concatenate([none, got], 0), jnp.concatenate([got[4:], got[:4], none], 0)
    )
    h = mid_taps(slab, mid_kernel)
    lo, hi = row_halo(h[0], h[2])
    middle = jax.nn.gelu(h[1] + lo.astype(F32) + hi.astype(F32)).astype(BF)

    slab_skip = to_slab(fine_halo(skip.transpose(2, 0, 1, 3), d), pick(skip_table[r]))

    middle, la, lb, slab_skip = lax.optimization_barrier((middle, la, lb, slab_skip))
    part = slab_call(skip_body, at, slab_skip, la, lb, split=False)

    packed = jnp.concatenate([middle, jnp.zeros((1, 64, 64), BF)], 0)
    packed = packed.reshape(3, 2, 64, 64).transpose(0, 2, 1, 3).reshape(3, 64, 128)
    got = lax.all_gather(packed, "col", axis=0)
    places = jnp.asarray(lift_table())
    rows = jnp.stack([places[jnp.clip(r + step, 0, 15), j] for step in (-1, 0, 1)])
    lift, for_next, for_prev = lift_planes(rows, got, up_kernel)

    lo, hi = row_halo(for_next, for_prev)
    keep, send = slab_call(last_body, at, lift, lo, hi, la, lb, part, full=True)
    out = jax.nn.gelu(reduce_tiles(keep, send, j)).astype(BF).reshape(8, 16, 2, 256)
    return out.transpose(2, 1, 0, 3)


def solution(mesh):
    cells = P("row", "col", "depth", None)
    rows = P(None, "row", None)
    return jax.shard_map(
        body,
        mesh=mesh,
        in_specs=(cells, rows, P(), P(None, None, "col"), P(), rows),
        out_specs=cells,
        check_vma=False,
    )
```

```python
import jax
import jax.numpy as jnp
import numpy as np
from jax import lax
from jax.experimental import pallas as pl
from jax.experimental.pallas import tpu as pltpu
from jax.sharding import PartitionSpec as P

BF = jnp.bfloat16
F32 = jnp.float32
ALL = ("row", "col", "depth")


def shards_of(r, j):
    zhi, x = r // 4, r % 4
    y, c = j // 2, j % 2
    s1 = ((zhi + c) % 4) * 4 + (x + y) % 4
    s2 = ((zhi + c + 2) % 4) * 4 + (x - y) % 4
    return s1, s2


def flat(r, j, d):
    return (r * 8 + j) * 2 + d


def shard_perms():
    p1, p2 = [], []
    for r in range(16):
        for j in range(8):
            for d in range(2):
                s1, s2 = shards_of(r, j)
                p1.append((flat(s1, j, d), flat(r, j, d)))
                p2.append((flat(s2, j, d if j % 2 else 1 - d), flat(r, j, d)))
    return p1, p2


def tables():
    first = np.zeros((16, 256), np.int32)
    skip = np.zeros((16, 256), np.int32)
    for r in range(16):
        for j in range(8):
            s1, s2 = shards_of(r, j)
            sk = (s2 if s1 < 8 else s1) - 8
            for i in range(16):
                first[r, 32 * j + i] = 16 * s1 + i
                first[r, 32 * j + 16 + i] = 16 * s2 + i
            for i in range(32):
                skip[r, 32 * j + i] = 32 * sk + i
    return first, skip


def lift_table():
    places = np.zeros((16, 8), np.int32)
    for r in range(16):
        for j in range(8):
            places[r, j] = min(shards_of(r, j))
    return places


def pick(table_row):
    want = jnp.tile(table_row.reshape(8, 1, 32), (1, 4, 1)).reshape(8, 128)
    want = want + (256 * (jnp.arange(128) // 32))[None, :]
    return (jnp.arange(1024)[:, None, None] == want[None]).astype(BF)


def edge_swap(face_lo, face_hi, d):
    send = jnp.where(d == 0, face_hi, face_lo)
    return lax.ppermute(send, "depth", [(0, 1), (1, 0)])


def row_halo(for_next, for_prev):
    lo = lax.ppermute(for_next, "row", [(i, i + 1) for i in range(15)])
    hi = lax.ppermute(for_prev, "row", [(i + 1, i) for i in range(15)])
    return lo, hi


def fine_halo(t, d):
    recv = edge_swap(t[:, 0], t[:, 7], d)
    t9 = jnp.concatenate([t, recv[:, None]], 1)
    lo, hi = row_halo(t9[1], t9[0])
    return jnp.stack([lo, t9[0], t9[1], hi])


def to_slab(t4, sel):
    rows = t4.reshape(4, 144, 256)
    sel = sel.reshape(4, 256, 8, 128)
    mixed = jnp.einsum("prc,pcjk->jrk", rows, sel, preferred_element_type=F32).astype(BF)
    got = lax.all_to_all(mixed, "col", 0, 0, tiled=True)
    return got


WHOLE = pl.BlockSpec(memory_space=pltpu.VMEM)
SCALARS = pl.BlockSpec(memory_space=pltpu.SMEM)


def fill_weights(tap, wt_ref):
    none = jnp.zeros((32, 256), BF)
    for blk in range(9):
        for p in range(4):
            for xo in range(2):
                rows = slice(128 * blk + 32 * p, 128 * blk + 32 * p + 32)
                value = tap(9 * (p - xo) + blk) if 0 <= p - xo <= 2 else none
                wt_ref[rows, 256 * xo : 256 * xo + 256] = value


def fill_plane(q, plane, patch_ref):
    y = lax.broadcasted_iota(jnp.int32, (128, 128), 0)
    shifted = (
        jnp.where(y == 0, 0.0, pltpu.roll(plane, 1, 0)),
        plane,
        jnp.where(y == 127, 0.0, pltpu.roll(plane, 127, 0)),
    )
    for b in range(3):
        value = shifted[b].astype(BF)
        for c in range(3):
            if 0 <= q - c < 8:
                rows = slice(128 * (q - c), 128 * (q - c) + 128)
                patch_ref[rows, 128 * (3 * b + c) : 128 * (3 * b + c) + 128] = value


def fill_from_exchange(d, got_ref, patch_ref):
    for z in range(9):
        plane = jnp.concatenate([got_ref[src, 16 * z : 16 * z + 16].astype(F32) for src in range(8)], 0)
        if z < 8:
            fill_plane(z + 1, plane, patch_ref)
        else:
            fill_plane(0, jnp.where(d == 1, plane, 0.0), patch_ref)
            fill_plane(9, jnp.where(d == 0, plane, 0.0), patch_ref)


def split_tiles(core, acc, keep_ref, send_ref):
    acc = acc.reshape(8, 128, 512)
    for y in range(4):
        first, second = acc[:, 32 * y : 32 * y + 16], acc[:, 32 * y + 16 : 32 * y + 32]
        keep_ref[y] = jnp.where(core == 0, first, second)
        send_ref[y] = jnp.where(core == 0, second, first)


def first_body(at_ref, got_ref, wa_ref, wb_ref, keep_ref, send_ref, wt_ref, patch_ref):
    fill_weights(lambda n: jnp.concatenate([wa_ref[n], wb_ref[n]], 0), wt_ref)
    fill_from_exchange(at_ref[0], got_ref, patch_ref)
    acc = jnp.dot(patch_ref[...], wt_ref[...], preferred_element_type=F32)
    split_tiles(at_ref[1], acc, keep_ref, send_ref)


def skip_body(at_ref, got_ref, wa_ref, wb_ref, acc_ref, wt_ref, patch_ref):
    low = at_ref[2] == 1
    fill_weights(lambda n: jnp.where(low, wb_ref[n], wa_ref[n]), wt_ref)
    fill_from_exchange(at_ref[0], got_ref, patch_ref)
    acc_ref[...] = jnp.dot(patch_ref[...], wt_ref[...], preferred_element_type=F32)


def last_body(
    at_ref, lift_ref, lo_ref, hi_ref, wa_ref, wb_ref, part_ref, keep_ref, send_ref, wt_ref, patch_ref, full_ref
):
    low = at_ref[2] == 1
    d = at_ref[0]
    fill_weights(lambda n: jnp.where(low, wa_ref[n], wb_ref[n]), wt_ref)
    group = lax.broadcasted_iota(jnp.int32, (128, 128), 1) // 32
    for g in range(3):
        lo, hi = lo_ref[g].astype(F32), hi_ref[g].astype(F32)
        for k in range(4):
            plane = lift_ref[4 * g + k].astype(F32)
            left = pltpu.roll(lo, 128 - 32 * k, 1) if k else lo
            right = pltpu.roll(hi, 96 - 32 * k, 1) if k < 3 else hi
            full_ref[4 * g + k] = jnp.where(group == 0, left, jnp.where(group == 3, right, plane))
    for q in range(1, 9):
        fill_plane(q, full_ref[q - 1 + 2 * d], patch_ref)
    fill_plane(0, jnp.where(d == 1, full_ref[1], 0.0), patch_ref)
    fill_plane(9, jnp.where(d == 0, full_ref[8], 0.0), patch_ref)
    acc = part_ref[...] + jnp.dot(patch_ref[...], wt_ref[...], preferred_element_type=F32)
    split_tiles(at_ref[1], acc, keep_ref, send_ref)


def slab_call(kernel, at, *arrays, split=True, full=False):
    tiles = jax.ShapeDtypeStruct((4, 8, 16, 512), F32)
    return pl.pallas_call(
        kernel,
        in_specs=[SCALARS] + [WHOLE] * len(arrays),
        out_specs=[WHOLE] * 2 if split else WHOLE,
        out_shape=[tiles] * 2 if split else jax.ShapeDtypeStruct((1024, 512), F32),
        scratch_shapes=[pltpu.VMEM((1152, 512), BF), pltpu.VMEM((1024, 1152), BF)]
        + [pltpu.VMEM((12, 128, 128), F32)] * full,
        compiler_params=pltpu.CompilerParams(vmem_limit_bytes=32 << 20),
    )(at, *arrays)


def mid_body(slab_ref, w_hbm, prev_ref, own_ref, next_ref, w_ref, sems):
    copies = [
        pltpu.make_async_copy(w_hbm.at[pl.ds(9 * a, 9)], w_ref.at[pl.ds(9 * a, 9)], sems.at[a]) for a in range(3)
    ]
    for copy in copies:
        copy.start()
    y = lax.broadcasted_iota(jnp.int32, (320, 64), 0) % 64
    near = [slab_ref[c : c + 5].reshape(320, 512) for c in range(3)]
    for a, out in enumerate((prev_ref, own_ref, next_ref)):
        copies[a].wait()
        total = jnp.zeros((320, 64), F32)
        for b in range(3):
            g = jnp.zeros((320, 64), F32)
            for c in range(3):
                g = g + jnp.dot(near[c], w_ref[9 * a + 3 * b + c], preferred_element_type=F32)
            if b == 0:
                g = jnp.where(y == 0, 0.0, pltpu.roll(g, 1, 0))
            if b == 2:
                g = jnp.where(y == 63, 0.0, pltpu.roll(g, 319, 0))
            total = total + g
        out[...] = total.reshape(5, 64, 64).astype(out.dtype)


def mid_taps(slab, w):
    return pl.pallas_call(
        mid_body,
        in_specs=[WHOLE, pl.BlockSpec(memory_space=pl.ANY)],
        out_specs=[WHOLE] * 3,
        out_shape=[jax.ShapeDtypeStruct((5, 64, 64), t) for t in (BF, F32, BF)],
        scratch_shapes=[pltpu.VMEM((27, 512, 64), BF), pltpu.SemaphoreType.DMA((3,))],
        compiler_params=pltpu.CompilerParams(vmem_limit_bytes=24 << 20),
        name="mid_taps",
    )(slab, w)


def lift_body(at_ref, got_ref, up_ref, planes_ref, next_ref, prev_ref, w_ref, tmp_ref):
    w_ref[...] = jnp.zeros((1024, 1024), BF)
    ch = lax.broadcasted_iota(jnp.int32, (256, 128), 0)
    lane = lax.broadcasted_iota(jnp.int32, (256, 128), 1)
    part, within = lane // 32, lane % 32
    shard = jnp.where(part == 0, at_ref[0], jnp.where(part == 3, at_ref[2], at_ref[1]))
    hit = ch == 32 * shard + within
    upper = jnp.where(hit & (part < 2), 1.0, 0.0).astype(BF)
    lower = jnp.where(hit & (part >= 2), 1.0, 0.0).astype(BF)
    for tap in range(4):
        u = jnp.dot(up_ref[tap], upper, preferred_element_type=F32)
        u = u + jnp.dot(up_ref[4 + tap], lower, preferred_element_type=F32)
        u = u.astype(BF)
        for src in range(8):
            for h in range(2):
                rows = slice(128 * src + 64 * h, 128 * src + 64 * h + 64)
                w_ref[rows, 128 * (4 * h + tap) : 128 * (4 * h + tap) + 128] = u[64 * src : 64 * src + 64]
    got = jnp.concatenate(
        [jnp.concatenate([got_ref[src, g] for src in range(8)], 1) for g in range(3)], 0
    )
    out = jnp.dot(got, w_ref[...], preferred_element_type=F32)
    for g in range(3):
        for h in range(2):
            for b in range(2):
                for c in range(2):
                    piece = out[64 * g : 64 * g + 64, 128 * (4 * h + 2 * b + c) : 128 * (4 * h + 2 * b + c) + 128]
                    tmp_ref[2 * (2 * g + h) + c, pl.ds(b, 64, stride=2), :] = piece
    group = lax.broadcasted_iota(jnp.int32, (128, 128), 1) // 32
    for q in range(3):
        nxt = jnp.zeros((128, 128), F32)
        prv = jnp.zeros((128, 128), F32)
        for k in range(4):
            plane = tmp_ref[4 * q + k]
            planes_ref[4 * q + k] = plane.astype(BF)
            nxt = jnp.where(group == k, pltpu.roll(plane, (32 * k - 96) % 128, 1), nxt)
            prv = jnp.where(group == k, pltpu.roll(plane, 32 * k, 1) if k else plane, prv)
        next_ref[q] = nxt.astype(BF)
        prev_ref[q] = prv.astype(BF)


def lift_planes(at, got, up):
    return pl.pallas_call(
        lift_body,
        in_specs=[SCALARS, WHOLE, WHOLE],
        out_specs=[WHOLE] * 3,
        out_shape=[jax.ShapeDtypeStruct((n, 128, 128), BF) for n in (12, 3, 3)],
        scratch_shapes=[pltpu.VMEM((1024, 1024), BF), pltpu.VMEM((12, 128, 128), F32)],
        compiler_params=pltpu.CompilerParams(vmem_limit_bytes=24 << 20),
        name="lift_planes",
    )(at, got, up)


def reduce_tiles(keep, send, j):
    y = j // 2
    pair = keep + lax.ppermute(send, "col", [(i, i ^ 1) for i in range(8)])
    pair = jnp.roll(pair, -y, 0)
    total = pair[0]
    for o in (1, 3, 2):
        perm = [(2 * a + b, 2 * ((a + o) % 4) + b) for a in range(4) for b in range(2)]
        total = total + lax.ppermute(pair[o].astype(BF), "col", perm).astype(F32)
    return total


def body(volume, first_kernel, down_kernel, mid_kernel, up_kernel, last_kernel):
    r, j, d = (lax.axis_index(a) for a in ALL)
    p1, p2 = shard_perms()
    first_table, skip_table = (jnp.asarray(t) for t in tables())
    wa = lax.ppermute(first_kernel, ALL, p1)
    wb = lax.ppermute(first_kernel, ALL, p2)
    in_low = (r // 4 + j % 2) % 4 < 2

    tile = volume.transpose(0, 2, 1, 3)
    t4, last_kernel = lax.optimization_barrier((fine_halo(tile, d), last_kernel))
    la = lax.ppermute(last_kernel, ALL, p1)
    lb = lax.ppermute(last_kernel, ALL, p2)
    at = jnp.stack([d, j % 2, in_low.astype(jnp.int32)])
    got = to_slab(t4, pick(first_table[r]))
    keep, send = slab_call(first_body, at, got, wa, wb)
    skip = jax.nn.gelu(reduce_tiles(keep, send, j)).astype(BF).reshape(8, 16, 2, 256)

    cells = skip.reshape(4, 2, 8, 2, 2, 256)
    down = down_kernel.reshape(2, 2, 2, 256, 512)
    coarse = jax.nn.gelu(jnp.einsum("kcjbae,abceo->kjo", cells, down, preferred_element_type=F32)).astype(BF)
    send = jnp.where(d == 0, coarse[2:], coarse[:2])
    recv = lax.ppermute(send, "depth", [(0, 1), (1, 0)])
    got = lax.all_gather(jnp.concatenate([coarse, recv], 0), "col", axis=0)
    got = got.transpose(1, 0, 2, 3).reshape(6, 64, 512)
    none = jnp.zeros((1, 64, 512), BF)
    slab = jnp.where(
        d == 0, jnp.concatenate([none, got], 0), jnp.concatenate([got[4:], got[:4], none], 0)
    )
    h = mid_taps(slab, mid_kernel)
    lo, hi = row_halo(h[0], h[2])
    middle = jax.nn.gelu(h[1] + lo.astype(F32) + hi.astype(F32)).astype(BF)

    slab_skip = to_slab(fine_halo(skip.transpose(2, 0, 1, 3), d), pick(skip_table[r]))

    middle, la, lb = lax.optimization_barrier((middle, la, lb))
    part = slab_call(skip_body, at, slab_skip, la, lb, split=False)

    packed = jnp.concatenate([middle, jnp.zeros((1, 64, 64), BF)], 0)
    packed = packed.reshape(3, 2, 64, 64).transpose(0, 2, 1, 3).reshape(3, 64, 128)
    got = lax.all_gather(packed, "col", axis=0)
    places = jnp.asarray(lift_table())
    rows = jnp.stack([places[jnp.clip(r + step, 0, 15), j] for step in (-1, 0, 1)])
    lift, for_next, for_prev = lift_planes(rows, got, up_kernel)

    lo, hi = row_halo(for_next, for_prev)
    keep, send = slab_call(last_body, at, lift, lo, hi, la, lb, part, full=True)
    out = jax.nn.gelu(reduce_tiles(keep, send, j)).astype(BF).reshape(8, 16, 2, 256)
    return out.transpose(2, 1, 0, 3)


def solution(mesh):
    cells = P("row", "col", "depth", None)
    rows = P(None, "row", None)
    return jax.shard_map(
        body,
        mesh=mesh,
        in_specs=(cells, rows, P(), P(None, None, "col"), P(), rows),
        out_specs=cells,
        check_vma=False,
    )
```
